32 devices in a mesh: row: 4 (over x, core), col: 8 (over z, y).
Axes of the slice: x: 2, y: 2, z: 4, core: 2. Of those that a mesh axis runs over, the one named last changes fastest.
Arguments:
- vectors: float32 [32768, 768], P(('row', 'col')), may hold values from -6 to 6
- list_ids: int32 [32768], P(('row', 'col')), may hold values from 0 to 16383, as said below
- pq_codes: int32 [32768, 96], P(('row', 'col')), may hold values from 0 to 255
- fill_counts: int32 [32, 32], P(('row', 'col')), may hold values from 0 to 32, as said below
- centroids: float32 [16384, 768], P(('row', 'col')), may hold values from -6 to 6
- codebook: float32 [96, 8, 256], P('col'), may hold values from -6 to 6
Outputs:
- coded_err: float32 [32768], P(('row', 'col'))
- best_err: float32 [32768], P(('row', 'col'))
The draws below stay inside these ranges and needn't reach their ends.
Inputs may be any that keep to these rules, and one draw needn't show every extreme that they name: `list_ids`: slot s of device p lies in block s // 32, which belongs to owner device s // 32 (devices numbered row-major over row and col); it names a list of that owner, from (s // 32) * 512 to (s // 32 + 1) * 512 - 1. fill_counts[p, d] is the number of live slots at the head of device p's block for owner d; some owner receives 32 live slots from every device.
All inputs are finite; a program needn't handle non-finite values.
Results may differ from the reference program's by a relative error of at most 0.0003.
Values sent between devices are 32-bit elements; how exact they have to be, the bound alone decides.
A program may use at most 256 MiB of HBM per device.

```python
import jax
import jax.numpy as jnp
from jax import lax

D = 768
SUB = 8
M = 96
K = 256
LISTS_DEV = 512
LISTS = 16384
SLOTS_DEV = 1024
CAP = 32
ROWS = 32768
DEVICES = 32


def draw_list_ids(key, part):
    slot_index = jnp.arange(ROWS, dtype=jnp.int32) % SLOTS_DEV
    owner = slot_index // CAP
    local_list = jax.random.randint(jax.random.fold_in(key, 11), (ROWS,), 0, LISTS_DEV, dtype=jnp.int32)
    return owner * LISTS_DEV + local_list


def draw_fill_counts(key, part):
    key_hot = jax.random.fold_in(key, 21)
    key_fill = jax.random.fold_in(key, 22)
    shuffled = jax.random.permutation(key_hot, DEVICES)
    hot_rank = shuffled < max(1, DEVICES // 16)
    base_fill = jax.random.randint(key_fill, (DEVICES, DEVICES), 0, CAP + 1, dtype=jnp.int32)
    return jnp.where(hot_rank[None, :], CAP, base_fill).astype(jnp.int32)


def place_ends(drawn, rng, low, largest):
    spot = [jax.random.randint(jax.random.fold_in(rng, axis), (), 0, length) for axis, length in enumerate(drawn.shape)]
    main_axis = drawn.shape.index(max(drawn.shape))
    neighbour = spot[:main_axis] + [(spot[main_axis] + 1) % drawn.shape[main_axis]] + spot[main_axis + 1:]
    return drawn.at[tuple(spot)].set(low).at[tuple(neighbour)].set(largest)


def block_scale(rng, shape, split, low, top_value):
    loudness = 1.0
    for dim, blocks in split:
        heights = jax.random.uniform(jax.random.fold_in(jax.random.fold_in(rng, 6), dim), (blocks,), jnp.float32, low / len(split), top_value / len(split))
        loudness = loudness * jnp.repeat(jnp.exp(heights), shape[dim] // blocks).reshape((-1,) + (1,) * (len(shape) - 1 - dim))
    return loudness


def centred(key, shape, deviation, bound, cuts=(), kind=jnp.bfloat16):
    result = jax.random.normal(key, shape, jnp.float32) * deviation
    if len(cuts) > 0:
        result = block_scale(key, shape, cuts, -0.22, 0.18) * result
    return jnp.clip(result, min=-bound, max=bound).astype(kind)


def setup_inputs(seed: int = 0) -> dict:
    streams_of = jax.random.split(jax.random.key(seed), 7)
    return {
        "vectors": centred(streams_of[0], (ROWS, D), 1.0, 6.0, ((0, 32),), jnp.float32),
        "list_ids": draw_list_ids(jax.random.fold_in(streams_of[6], 71), 0),
        "pq_codes": place_ends(jax.random.randint(streams_of[2], (ROWS, M), 0, K), jax.random.fold_in(streams_of[2], 1), 0, K - 1).astype(jnp.int32),
        "fill_counts": draw_fill_counts(jax.random.fold_in(streams_of[6], 71), 0),
        "centroids": centred(streams_of[4], (LISTS, D), 1.0, 6.0, ((0, 32),), jnp.float32),
        "codebook": centred(streams_of[5], (M, SUB, K), 1.0, 6.0, ((0, 8),), jnp.float32),
    }


def block_terms(block_vec, block_codes, codebook, code_norms):
    resid_norms = jnp.sum(block_vec * block_vec, axis=2)
    cross_term = jnp.einsum("bms,msk->bmk", block_vec, codebook, precision=lax.Precision.HIGHEST)
    dist_table = resid_norms[:, :, None] - 2.0 * cross_term + code_norms[None, :, :]
    best_sum = jnp.sum(jnp.min(dist_table, axis=2), axis=1)
    code_index = lax.broadcasted_iota(jnp.int32, dist_table.shape, 2)
    coded_sum = jnp.sum(jnp.where(code_index == block_codes[:, :, None], dist_table, 0.0), axis=(1, 2))
    return jnp.stack([coded_sum, best_sum])


def reference(vectors, list_ids, pq_codes, fill_counts, centroids, codebook):
    device_count = fill_counts.shape[0]
    slot_count = vectors.shape[0] // device_count
    capacity = slot_count // device_count
    sub_count = pq_codes.shape[1]
    sub_width = vectors.shape[1] // sub_count
    block_rows = 256
    block_count = slot_count // block_rows
    code_norms = jnp.sum(codebook * codebook, axis=1)

    def one_device(inputs):
        device_vec, device_ids, device_codes = inputs
        residual = device_vec - jnp.take(centroids, device_ids, axis=0)
        shaped = residual.reshape(block_count, block_rows, sub_count, sub_width)
        shaped_codes = device_codes.reshape(block_count, block_rows, sub_count)

        def one_block(pair):
            return block_terms(pair[0], pair[1], codebook, code_norms)

        parts = lax.map(one_block, (shaped, shaped_codes))
        return jnp.transpose(parts, (1, 0, 2)).reshape(2, slot_count)

    results = lax.map(one_device, (vectors.reshape(device_count, slot_count, -1), list_ids.reshape(device_count, slot_count), pq_codes.reshape(device_count, slot_count, sub_count)))
    slot_pos = jnp.arange(capacity, dtype=jnp.int32)
    live_mask = (slot_pos[None, None, :] < fill_counts[:, :, None]).reshape(device_count, slot_count)
    coded_err = jnp.where(live_mask, results[:, 0, :], 0.0).reshape(-1)
    best_err = jnp.where(live_mask, results[:, 1, :], 0.0).reshape(-1)
    return coded_err, best_err
```

```python
import functools

import jax
import jax.numpy as jnp
from jax import lax
from jax.experimental import pallas as pl
from jax.experimental.pallas import tpu as pltpu
from jax.sharding import PartitionSpec as P

F32 = jnp.float32
BF16 = jnp.bfloat16
DEPTH = 64


def split3(x):
    hi = x.astype(BF16).astype(F32)
    rest = x - hi
    mid = rest.astype(BF16).astype(F32)
    return hi, mid, rest - mid


def build_table(cb_ref, w_ref):
    sub_count, sub_width, code_count = cb_ref.shape

    def step(m, carry):
        c = cb_ref[m]
        hi, mid, lo = split3(-2.0 * c)
        norm = jnp.sum(c * c, axis=0, keepdims=True)
        nh, nm, nl = split3(norm)
        line = lax.broadcasted_iota(jnp.int32, c.shape, 0)
        norms = jnp.where(line == 0, nh, jnp.where(line == 1, nm, jnp.where(line == 2, nl, 0.0)))
        pieces = [hi, hi, hi, mid, mid, lo, norms, jnp.zeros_like(c)]
        w_ref[m] = jnp.concatenate(pieces, axis=0).T.astype(BF16)
        return carry

    lax.fori_loop(0, sub_count, step, 0, unroll=4)


def pick(row, code, sub_width):
    lanes = code.shape[1]
    outs = []
    for start in range(0, lanes, 128):
        idx = jnp.broadcast_to(code[:, start:start + 128], (sub_width, 128))
        low = jnp.bitwise_and(idx, 127)
        got = None
        for part in range(row.shape[1] // 128):
            piece = jnp.take_along_axis(
                row[:, part * 128:(part + 1) * 128], low, axis=1, mode="promise_in_bounds"
            )
            got = piece if got is None else jnp.where(idx >= part * 128, piece, got)
        outs.append(got)
    return jnp.concatenate(outs, axis=1)


def score(rt_ref, codes_ref, cb_ref, w_ref, unroll):
    sub_count, sub_width, code_count = cb_ref.shape
    width = rt_ref.shape[1]
    ones = jnp.ones((sub_width, width), F32)
    zeros = jnp.zeros((sub_width, width), F32)

    def step(m, carry):
        coded, norm, best = carry
        r = rt_ref[pl.ds(pl.multiple_of(m * sub_width, sub_width), sub_width), :]
        hi, mid, lo = split3(r)
        x = jnp.concatenate([hi, mid, lo, hi, mid, hi, ones, zeros], axis=0).astype(BF16)
        table = jnp.dot(w_ref[m], x, preferred_element_type=F32)
        best = best + jnp.min(table, axis=0, keepdims=True)
        norm = norm + r * r
        diff = r - pick(cb_ref[m], codes_ref[pl.ds(m, 1), :], sub_width)
        return coded + diff * diff, norm, best

    coded, norm, best = lax.fori_loop(
        0, sub_count, step, (zeros, zeros, jnp.zeros((1, width), F32)), unroll=unroll
    )
    coded = jnp.sum(coded, axis=0, keepdims=True)
    best = best + jnp.sum(norm, axis=0, keepdims=True)
    return coded, best


def score_kernel(v_ref, c_ref, codes_ref, cb_ref, w_ref, coded_ref, best_ref, rt_ref):
    rt_ref[...] = (v_ref[...] - c_ref[...]).T
    coded, best = score(rt_ref, codes_ref, cb_ref, w_ref, 4)
    coded_ref[...] = coded
    best_ref[...] = best


def local(vectors, list_ids, pq_codes, fill_counts, centroids, codebook):
    row_count = lax.axis_size("row")
    col_count = lax.axis_size("col")
    device_count = row_count * col_count
    slot_count, feature_width = vectors.shape
    capacity = slot_count // device_count
    sub_total = pq_codes.shape[1]
    sub_width, code_count = codebook.shape[1:]
    axes = ("row", "col")
    swap = functools.partial(lax.all_to_all, axis_name=axes, split_axis=0, concat_axis=0, tiled=True)

    got_ids = swap(list_ids.reshape(device_count, capacity)).reshape(slot_count)
    wanted = jnp.take(centroids, got_ids % centroids.shape[0], axis=0, mode="clip")
    share = sub_width // row_count
    mine = lax.dynamic_slice_in_dim(codebook, lax.axis_index("row") * share, share, axis=1)
    mine = lax.all_gather(mine, "col", axis=0, tiled=True)
    book = lax.all_gather(mine, "row", axis=1, tiled=True)
    got_cent = swap(wanted.reshape(device_count, capacity, feature_width)).reshape(slot_count, feature_width)
    codes_t = pq_codes.T

    table = pl.pallas_call(
        build_table,
        out_shape=jax.ShapeDtypeStruct((sub_total, code_count, DEPTH), BF16),
        in_specs=[pl.BlockSpec(memory_space=pltpu.VMEM)],
        out_specs=pl.BlockSpec(memory_space=pltpu.VMEM),
        cost_estimate=pl.CostEstimate(flops=10**8, bytes_accessed=20_000_000, transcendentals=0),
        name="build_table",
    )(book)

    width = 256
    whole3 = lambda i: (0, 0, 0)
    coded, best = pl.pallas_call(
        score_kernel,
        grid=(slot_count // width,),
        out_shape=[jax.ShapeDtypeStruct((1, slot_count), F32)] * 2,
        in_specs=[
            pl.BlockSpec((width, feature_width), lambda i: (i, 0)),
            pl.BlockSpec((width, feature_width), lambda i: (i, 0)),
            pl.BlockSpec((sub_total, width), lambda i: (0, i)),
            pl.BlockSpec((sub_total, sub_width, code_count), whole3),
            pl.BlockSpec((sub_total, code_count, DEPTH), whole3),
        ],
        out_specs=[pl.BlockSpec((1, width), lambda i: (0, i))] * 2,
        scratch_shapes=[pltpu.VMEM((feature_width, width), F32)],
        name="score",
    )(vectors, got_cent, codes_t, book, table)

    slot_pos = jnp.arange(capacity, dtype=jnp.int32)
    live = (slot_pos[None, :] < fill_counts[0][:, None]).reshape(slot_count)
    coded_err = jnp.where(live, coded.reshape(slot_count), 0.0)
    best_err = jnp.where(live, best.reshape(slot_count), 0.0)
    return (coded_err, best_err)


def solution(mesh):
    in_specs = (
        P(("row", "col"), None),
        P(("row", "col")),
        P(("row", "col"), None),
        P(("row", "col"), None),
        P(("row", "col"), None),
        P("col", None, None),
    )
    out_specs = (P(("row", "col")), P(("row", "col")))
    return jax.shard_map(local, mesh=mesh, in_specs=in_specs, out_specs=out_specs, check_vma=False)
```

```python
import functools

import jax
import jax.numpy as jnp
from jax import lax
from jax.experimental import pallas as pl
from jax.experimental.pallas import tpu as pltpu
from jax.sharding import PartitionSpec as P

F32 = jnp.float32
BF16 = jnp.bfloat16
DEPTH = 64


def split3(x):
    hi = x.astype(BF16).astype(F32)
    rest = x - hi
    mid = rest.astype(BF16).astype(F32)
    return hi, mid, rest - mid


def build_table(cb_ref, w_ref):
    sub_count, sub_width, code_count = cb_ref.shape

    def step(m, carry):
        c = cb_ref[m]
        hi, mid, lo = split3(-2.0 * c)
        norm = jnp.sum(c * c, axis=0, keepdims=True)
        nh, nm, nl = split3(norm)
        line = lax.broadcasted_iota(jnp.int32, c.shape, 0)
        norms = jnp.where(line == 0, nh, jnp.where(line == 1, nm, jnp.where(line == 2, nl, 0.0)))
        pieces = [hi, hi, hi, mid, mid, lo, norms, jnp.zeros_like(c)]
        w_ref[m] = jnp.concatenate(pieces, axis=0).T.astype(BF16)
        return carry

    lax.fori_loop(0, sub_count, step, 0, unroll=4)


def pick(row, code, sub_width):
    lanes = code.shape[1]
    outs = []
    for start in range(0, lanes, 128):
        idx = jnp.broadcast_to(code[:, start:start + 128], (sub_width, 128))
        low = jnp.bitwise_and(idx, 127)
        got = None
        for part in range(row.shape[1] // 128):
            piece = jnp.take_along_axis(
                row[:, part * 128:(part + 1) * 128], low, axis=1, mode="promise_in_bounds"
            )
            got = piece if got is None else jnp.where(idx >= part * 128, piece, got)
        outs.append(got)
    return jnp.concatenate(outs, axis=1)


def score(rt_ref, codes_ref, cb_ref, w_ref):
    sub_count, sub_width, code_count = cb_ref.shape
    width = rt_ref.shape[1]
    ones = jnp.ones((sub_width, width), F32)
    zeros = jnp.zeros((sub_width, width), F32)

    def step(g, carry):
        coded, norm, best = carry
        codes = codes_ref[pl.ds(pl.multiple_of(g * 8, 8), 8), :]
        for i in range(8):
            m = g * 8 + i
            r = rt_ref[pl.ds(pl.multiple_of(m * sub_width, sub_width), sub_width), :]
            hi, mid, lo = split3(r)
            x = jnp.concatenate([hi, mid, lo, hi, mid, hi, ones, zeros], axis=0).astype(BF16)
            table = jnp.dot(w_ref[m], x, preferred_element_type=F32)
            best = best + jnp.min(table, axis=0, keepdims=True)
            norm = norm + r * r
            diff = r - pick(cb_ref[m], codes[i:i + 1, :], sub_width)
            coded = coded + diff * diff
        return coded, norm, best

    coded, norm, best = lax.fori_loop(
        0, sub_count // 8, step, (zeros, zeros, jnp.zeros((1, width), F32))
    )
    coded = jnp.sum(coded, axis=0, keepdims=True)
    best = best + jnp.sum(norm, axis=0, keepdims=True)
    return coded, best


def exchange_kernel(row_count, col_count, wanted_ref, cb_ref, v_ref, codes_ref, coded_ref, best_ref,
                    got_ref, book_ref, w_ref, rt_ref, first_send, second_send, book_recv, rows_send, rows_recv):
    row = lax.axis_index("row")
    col = lax.axis_index("col")
    sub_local = cb_ref.shape[0]
    width = rt_ref.shape[1]
    capacity = width // col_count
    groups = col_count // row_count

    def other_row(step):
        return lax.rem(row + step + row_count, row_count)

    def other_col(step):
        return lax.rem(col + step + col_count, col_count)

    def piece(j):
        return book_ref.at[pl.ds(j * sub_local, sub_local)]

    def block(ref, r, c):
        start = pl.multiple_of((r * col_count + c) * capacity, capacity)
        return ref.at[pl.ds(start, capacity)]

    def first_copy(step):
        return pltpu.make_async_remote_copy(
            src_ref=cb_ref, dst_ref=piece(col), send_sem=first_send.at[step], recv_sem=book_recv.at[col],
            device_id=(row, other_col(step)), device_id_type=pl.DeviceIdType.MESH)

    def second_copy(group, step):
        j = group * row_count + row
        return pltpu.make_async_remote_copy(
            src_ref=piece(j), dst_ref=piece(j), send_sem=second_send.at[group, step], recv_sem=book_recv.at[j],
            device_id=(other_row(step), col), device_id_type=pl.DeviceIdType.MESH)

    def arrived(j):
        return pltpu.make_async_remote_copy(
            src_ref=cb_ref, dst_ref=piece(j), send_sem=first_send.at[0], recv_sem=book_recv.at[j],
            device_id=(row, other_col(1)), device_id_type=pl.DeviceIdType.MESH)

    def rows_copy(row_step, col_step):
        r, c = other_row(row_step), other_col(col_step)
        slot = row_step * col_count + col_step
        return pltpu.make_async_remote_copy(
            src_ref=block(wanted_ref, r, c), dst_ref=block(got_ref, row, col),
            send_sem=rows_send.at[slot], recv_sem=rows_recv.at[slot],
            device_id=(r, c), device_id_type=pl.DeviceIdType.MESH)

    def rows_arrived(row_step, col_step):
        r, c = other_row(-row_step), other_col(-col_step)
        slot = row_step * col_count + col_step
        return pltpu.make_async_remote_copy(
            src_ref=block(wanted_ref, r, c), dst_ref=block(got_ref, r, c),
            send_sem=rows_send.at[slot], recv_sem=rows_recv.at[slot],
            device_id=(other_row(row_step), other_col(col_step)), device_id_type=pl.DeviceIdType.MESH)

    spreads = lax.rem(col, row_count) == row

    @pl.when(spreads)
    def _():
        for step in range(1, col_count):
            first_copy(step).start()

    book_ref[pl.ds(col * sub_local, sub_local)] = cb_ref[...]
    own = pl.multiple_of((row * col_count + col) * capacity, capacity)
    got_ref[pl.ds(own, capacity), :] = wanted_ref[pl.ds(own, capacity), :]
    for group in range(groups):
        @pl.when(group * row_count + row != col)
        def _(group=group):
            arrived(group * row_count + row).wait_recv()
            for step in range(1, row_count):
                second_copy(group, step).start()

    pairs = [(a, b) for a in range(row_count) for b in range(col_count) if a + b > 0]
    for a, b in pairs:
        rows_copy(a, b).start()

    for group in range(groups):
        for step in range(1, row_count):
            j = group * row_count + other_row(-step)

            @pl.when(j != col)
            def _(j=j):
                arrived(j).wait_recv()
    build_table(book_ref, w_ref)

    for a in range(row_count):
        for b in range(col_count):
            if a + b > 0:
                rows_arrived(a, b).wait_recv()
        base = pl.multiple_of(other_row(-a) * width, width)
        rt_ref[...] = (v_ref[pl.ds(base, width), :] - got_ref[pl.ds(base, width), :]).T
        coded, best = score(rt_ref, codes_ref.at[:, pl.ds(base, width)], book_ref, w_ref)
        coded_ref[:, pl.ds(base, width)] = coded
        best_ref[:, pl.ds(base, width)] = best

    @pl.when(spreads)
    def _():
        for step in range(1, col_count):
            first_copy(step).wait_send()

    for group in range(groups):
        @pl.when(group * row_count + row != col)
        def _(group=group):
            for step in range(1, row_count):
                second_copy(group, step).wait_send()
    for a, b in pairs:
        rows_copy(a, b).wait_send()


def local(vectors, list_ids, pq_codes, fill_counts, centroids, codebook):
    row_count = lax.axis_size("row")
    col_count = lax.axis_size("col")
    device_count = row_count * col_count
    slot_count, feature_width = vectors.shape
    capacity = slot_count // device_count
    sub_total = pq_codes.shape[1]
    sub_width, code_count = codebook.shape[1:]
    axes = ("row", "col")
    swap = functools.partial(lax.all_to_all, axis_name=axes, split_axis=0, concat_axis=0, tiled=True)

    got_ids = swap(list_ids.reshape(device_count, capacity)).reshape(slot_count)
    wanted = jnp.take(centroids, got_ids % centroids.shape[0], axis=0, mode="clip")
    width = slot_count // row_count
    vmem = pl.BlockSpec(memory_space=pltpu.VMEM)
    coded, best = pl.pallas_call(
        functools.partial(exchange_kernel, row_count, col_count),
        out_shape=[jax.ShapeDtypeStruct((1, slot_count), F32)] * 2,
        in_specs=[vmem] * 4,
        out_specs=[vmem] * 2,
        scratch_shapes=[
            pltpu.VMEM((slot_count, feature_width), F32),
            pltpu.VMEM((sub_total, sub_width, code_count), F32),
            pltpu.VMEM((sub_total, code_count, DEPTH), BF16),
            pltpu.VMEM((feature_width, width), F32),
            pltpu.SemaphoreType.DMA((col_count,)),
            pltpu.SemaphoreType.DMA((col_count // row_count, row_count)),
            pltpu.SemaphoreType.DMA((col_count,)),
            pltpu.SemaphoreType.DMA((device_count,)),
            pltpu.SemaphoreType.DMA((device_count,)),
        ],
        compiler_params=pltpu.CompilerParams(has_side_effects=True, vmem_limit_bytes=48 * 2**20),
        name="exchange_score",
    )(wanted, codebook, vectors, pq_codes.T)

    slot_pos = jnp.arange(capacity, dtype=jnp.int32)
    live = (slot_pos[None, :] < fill_counts[0][:, None]).reshape(slot_count)
    coded_err = jnp.where(live, coded.reshape(slot_count), 0.0)
    best_err = jnp.where(live, best.reshape(slot_count), 0.0)
    return (coded_err, best_err)


def solution(mesh):
    in_specs = (
        P(("row", "col"), None),
        P(("row", "col")),
        P(("row", "col"), None),
        P(("row", "col"), None),
        P(("row", "col"), None),
        P("col", None, None),
    )
    out_specs = (P(("row", "col")), P(("row", "col")))
    return jax.shard_map(local, mesh=mesh, in_specs=in_specs, out_specs=out_specs, check_vma=False)
```

```python
import functools

import jax
import jax.numpy as jnp
from jax import lax
from jax.experimental import pallas as pl
from jax.experimental.pallas import tpu as pltpu
from jax.sharding import PartitionSpec as P

F32 = jnp.float32
BF16 = jnp.bfloat16
DEPTH = 64


def split3(x):
    hi = x.astype(BF16).astype(F32)
    rest = x - hi
    mid = rest.astype(BF16).astype(F32)
    return hi, mid, rest - mid


def build_table(cb_ref, w_ref):
    sub_count, sub_width, code_count = cb_ref.shape

    def step(m, carry):
        c = cb_ref[m]
        hi, mid, lo = split3(-2.0 * c)
        norm = jnp.sum(c * c, axis=0, keepdims=True)
        nh, nm, nl = split3(norm)
        line = lax.broadcasted_iota(jnp.int32, c.shape, 0)
        norms = jnp.where(line == 0, nh, jnp.where(line == 1, nm, jnp.where(line == 2, nl, 0.0)))
        pieces = [hi, hi, hi, mid, mid, lo, norms, jnp.zeros_like(c)]
        w_ref[m] = jnp.concatenate(pieces, axis=0).T.astype(BF16)
        return carry

    lax.fori_loop(0, sub_count, step, 0, unroll=4)


def pick(row, code, sub_width):
    lanes = code.shape[1]
    outs = []
    for start in range(0, lanes, 128):
        idx = jnp.broadcast_to(code[:, start:start + 128], (sub_width, 128))
        low = jnp.bitwise_and(idx, 127)
        got = None
        for part in range(row.shape[1] // 128):
            piece = jnp.take_along_axis(
                row[:, part * 128:(part + 1) * 128], low, axis=1, mode="promise_in_bounds"
            )
            got = piece if got is None else jnp.where(idx >= part * 128, piece, got)
        outs.append(got)
    return jnp.concatenate(outs, axis=1)


def score(rt_ref, codes_ref, cb_ref, w_ref):
    sub_count, sub_width, code_count = cb_ref.shape
    width = rt_ref.shape[1]
    ones = jnp.ones((sub_width, width), F32)
    zeros = jnp.zeros((sub_width, width), F32)

    def step(g, carry):
        coded, norm, best = carry
        codes = codes_ref[pl.ds(pl.multiple_of(g * 8, 8), 8), :]
        for i in range(8):
            m = g * 8 + i
            r = rt_ref[pl.ds(pl.multiple_of(m * sub_width, sub_width), sub_width), :]
            hi, mid, lo = split3(r)
            x = jnp.concatenate([hi, mid, lo, hi, mid, hi, ones, zeros], axis=0).astype(BF16)
            table = jnp.dot(w_ref[m], x, preferred_element_type=F32)
            best = best + jnp.min(table, axis=0, keepdims=True)
            norm = norm + r * r
            diff = r - pick(cb_ref[m], codes[i:i + 1, :], sub_width)
            coded = coded + diff * diff
        return coded, norm, best

    coded, norm, best = lax.fori_loop(
        0, sub_count // 8, step, (zeros, zeros, jnp.zeros((1, width), F32))
    )
    coded = jnp.sum(coded, axis=0, keepdims=True)
    best = best + jnp.sum(norm, axis=0, keepdims=True)
    return coded, best


def exchange_kernel(row_count, col_count, wanted_ref, cb_ref, v_ref, codes_ref, coded_ref, best_ref,
                    got_ref, book_ref, w_ref, rt_ref, first_send, second_send, book_recv, rows_send, rows_recv):
    row = lax.axis_index("row")
    col = lax.axis_index("col")
    sub_local = cb_ref.shape[0]
    width = rt_ref.shape[1]
    capacity = width // col_count
    groups = col_count // row_count

    def other_row(step):
        return lax.rem(row + step + row_count, row_count)

    def other_col(step):
        return lax.rem(col + step + col_count, col_count)

    def piece(j):
        return book_ref.at[pl.ds(j * sub_local, sub_local)]

    def block(ref, r, c):
        start = pl.multiple_of((r * col_count + c) * capacity, capacity)
        return ref.at[pl.ds(start, capacity)]

    def first_copy(step):
        return pltpu.make_async_remote_copy(
            src_ref=cb_ref, dst_ref=piece(col), send_sem=first_send.at[step], recv_sem=book_recv.at[col],
            device_id=(row, other_col(step)), device_id_type=pl.DeviceIdType.MESH)

    def second_copy(group, step):
        j = group * row_count + row
        return pltpu.make_async_remote_copy(
            src_ref=piece(j), dst_ref=piece(j), send_sem=second_send.at[group, step], recv_sem=book_recv.at[j],
            device_id=(other_row(step), col), device_id_type=pl.DeviceIdType.MESH)

    def arrived(j):
        return pltpu.make_async_remote_copy(
            src_ref=cb_ref, dst_ref=piece(j), send_sem=first_send.at[0], recv_sem=book_recv.at[j],
            device_id=(row, other_col(1)), device_id_type=pl.DeviceIdType.MESH)

    def rows_copy(row_step, col_step):
        r, c = other_row(row_step), other_col(col_step)
        slot = row_step * col_count + col_step
        return pltpu.make_async_remote_copy(
            src_ref=block(wanted_ref, r, c), dst_ref=block(got_ref, row, col),
            send_sem=rows_send.at[slot], recv_sem=rows_recv.at[slot],
            device_id=(r, c), device_id_type=pl.DeviceIdType.MESH)

    def rows_arrived(row_step, col_step):
        r, c = other_row(-row_step), other_col(-col_step)
        slot = row_step * col_count + col_step
        return pltpu.make_async_remote_copy(
            src_ref=block(wanted_ref, r, c), dst_ref=block(got_ref, r, c),
            send_sem=rows_send.at[slot], recv_sem=rows_recv.at[slot],
            device_id=(other_row(row_step), other_col(col_step)), device_id_type=pl.DeviceIdType.MESH)

    spreads = lax.rem(col, row_count) == row

    @pl.when(spreads)
    def _():
        for step in range(1, col_count):
            first_copy(step).start()

    book_ref[pl.ds(col * sub_local, sub_local)] = cb_ref[...]
    own = pl.multiple_of((row * col_count + col) * capacity, capacity)
    got_ref[pl.ds(own, capacity), :] = wanted_ref[pl.ds(own, capacity), :]
    for group in range(groups):
        @pl.when(group * row_count + row != col)
        def _(group=group):
            arrived(group * row_count + row).wait_recv()
            for step in range(1, row_count):
                second_copy(group, step).start()

    pairs = [(a, b) for a in range(row_count) for b in range(col_count) if a + b > 0]
    for a, b in pairs:
        rows_copy(a, b).start()

    for group in range(groups):
        for step in range(1, row_count):
            j = group * row_count + other_row(-step)

            @pl.when(j != col)
            def _(j=j):
                arrived(j).wait_recv()
    build_table(book_ref, w_ref)

    for a in range(row_count):
        for b in range(col_count):
            if a + b > 0:
                rows_arrived(a, b).wait_recv()
        base = pl.multiple_of(other_row(-a) * width, width)
        rt_ref[...] = (v_ref[pl.ds(base, width), :] - got_ref[pl.ds(base, width), :]).T
        coded, best = score(rt_ref, codes_ref.at[:, pl.ds(base, width)], book_ref, w_ref)
        coded_ref[:, pl.ds(base, width)] = coded
        best_ref[:, pl.ds(base, width)] = best

    @pl.when(spreads)
    def _():
        for step in range(1, col_count):
            first_copy(step).wait_send()

    for group in range(groups):
        @pl.when(group * row_count + row != col)
        def _(group=group):
            for step in range(1, row_count):
                second_copy(group, step).wait_send()
    for a, b in pairs:
        rows_copy(a, b).wait_send()


def ids_kernel(row_count, col_count, ids_ref, out_ref, land_ref, send, recv):
    row = lax.axis_index("row")
    col = lax.axis_index("col")
    me = row * col_count + col

    def other(a, b):
        return lax.rem(row + a + row_count, row_count), lax.rem(col + b + col_count, col_count)

    def copy(a, b, back):
        r, c = other(a, b)
        fr, fc = other(-a, -b)
        slot = a * col_count + b
        return pltpu.make_async_remote_copy(
            src_ref=ids_ref.at[r * col_count + c],
            dst_ref=land_ref.at[fr * col_count + fc if back else me],
            send_sem=send.at[slot], recv_sem=recv.at[slot],
            device_id=(r, c), device_id_type=pl.DeviceIdType.MESH)

    pairs = [(a, b) for a in range(row_count) for b in range(col_count) if a + b > 0]
    for a, b in pairs:
        copy(a, b, False).start()
    land_ref[me] = ids_ref[me]
    for a, b in pairs:
        copy(a, b, True).wait_recv()
    out_ref[...] = land_ref[...]
    for a, b in pairs:
        copy(a, b, False).wait_send()


def local(vectors, list_ids, pq_codes, fill_counts, centroids, codebook):
    row_count = lax.axis_size("row")
    col_count = lax.axis_size("col")
    device_count = row_count * col_count
    slot_count, feature_width = vectors.shape
    capacity = slot_count // device_count
    sub_total = pq_codes.shape[1]
    sub_width, code_count = codebook.shape[1:]
    vmem = pl.BlockSpec(memory_space=pltpu.VMEM)
    ids_shape = (device_count, 1, capacity)
    got_ids = pl.pallas_call(
        functools.partial(ids_kernel, row_count, col_count),
        out_shape=jax.ShapeDtypeStruct(ids_shape, jnp.int32),
        in_specs=[vmem],
        out_specs=vmem,
        scratch_shapes=[
            pltpu.VMEM(ids_shape, jnp.int32),
            pltpu.SemaphoreType.DMA((device_count,)),
            pltpu.SemaphoreType.DMA((device_count,)),
        ],
        compiler_params=pltpu.CompilerParams(has_side_effects=True),
        name="exchange_ids",
    )(list_ids.reshape(ids_shape)).reshape(slot_count)
    lines = lax.rem(got_ids, centroids.shape[0])
    wanted = centroids.at[lines].get(mode="promise_in_bounds", wrap_negative_indices=False)
    width = slot_count // row_count
    coded, best = pl.pallas_call(
        functools.partial(exchange_kernel, row_count, col_count),
        out_shape=[jax.ShapeDtypeStruct((1, slot_count), F32)] * 2,
        in_specs=[vmem] * 4,
        out_specs=[vmem] * 2,
        scratch_shapes=[
            pltpu.VMEM((slot_count, feature_width), F32),
            pltpu.VMEM((sub_total, sub_width, code_count), F32),
            pltpu.VMEM((sub_total, code_count, DEPTH), BF16),
            pltpu.VMEM((feature_width, width), F32),
            pltpu.SemaphoreType.DMA((col_count,)),
            pltpu.SemaphoreType.DMA((col_count // row_count, row_count)),
            pltpu.SemaphoreType.DMA((col_count,)),
            pltpu.SemaphoreType.DMA((device_count,)),
            pltpu.SemaphoreType.DMA((device_count,)),
        ],
        compiler_params=pltpu.CompilerParams(has_side_effects=True, vmem_limit_bytes=48 * 2**20),
        name="exchange_score",
    )(wanted, codebook, vectors, pq_codes.T)

    slot_pos = jnp.arange(capacity, dtype=jnp.int32)
    live = (slot_pos[None, :] < fill_counts[0][:, None]).reshape(slot_count)
    coded_err = jnp.where(live, coded.reshape(slot_count), 0.0)
    best_err = jnp.where(live, best.reshape(slot_count), 0.0)
    return (coded_err, best_err)


def solution(mesh):
    in_specs = (
        P(("row", "col"), None),
        P(("row", "col")),
        P(("row", "col"), None),
        P(("row", "col"), None),
        P(("row", "col"), None),
        P("col", None, None),
    )
    out_specs = (P(("row", "col")), P(("row", "col")))
    return jax.shard_map(local, mesh=mesh, in_specs=in_specs, out_specs=out_specs, check_vma=False)
```
